32 devices in a mesh: gy: 8 (over z, x), gx: 4 (over y, core).
Axes of the slice: x: 2, y: 2, z: 4, core: 2. Of those that a mesh axis runs over, the one named last changes fastest.
Arguments:
- ensemble: bfloat16 [32, 2, 512, 512], P(None, None, 'gy', 'gx'), may hold values from -1.1953125 to 1.1953125
- obs_cell: int32 [8, 4, 2048], P('gy', 'gx'), may hold values from 0 to 8191
- obs_level: int32 [8, 4, 2048], P('gy', 'gx'), may hold values from 0 to 1
- innovation: float32 [8, 4, 2048], P('gy', 'gx'), may hold values from -6 to 6
- obs_weight: float32 [8, 4, 2048], P('gy', 'gx'), may hold values from 0.5 to 4
Outputs:
- control: float32 [32, 2, 512, 512], P(None, None, 'gy', 'gx')
- increment: float32 [2, 512, 512], P(None, 'gy', 'gx')
The draws below stay inside these ranges and needn't reach their ends.
Inputs may be any that keep to these rules, and one draw needn't show every extreme that they name: obs_cell holds row * 128 + column of the observation within its device's block of 64 x 128 cells.
All inputs are finite; a program needn't handle non-finite values.
Results may differ from the reference program's by a relative error of at most 0.0003.
Values sent between devices are 32-bit elements; how exact they have to be, the bound alone decides.
A program may use at most 128 MiB of HBM per device.

```python
import math
import jax
import jax.numpy as jnp
from jax import lax

MEMBERS = 32
LEV = 2
SWEEPS = 4
CY = 64
CX = 128
OBS_DEV = 2048
NY = 512
NX = 512
N_GY = 8
N_GX = 4


def place_ends(result, key, smallest, high):
    dims = result.shape
    place = [jax.random.randint(jax.random.fold_in(key, axis), (), 0, dims[axis]) for axis in range(len(dims))]
    result = result.at[tuple(place)].set(smallest)
    longest = dims.index(max(dims))
    place[longest] = (place[longest] + 1) % dims[longest]
    return result.at[tuple(place)].set(high)


def block_scale(stream_key, dims, split, low, top_value):
    level = 1.0
    for axis_at, parts in split:
        draws = jax.random.uniform(jax.random.fold_in(jax.random.fold_in(stream_key, 6), axis_at), (parts,), jnp.float32, low / len(split), top_value / len(split))
        level = level * jnp.repeat(jnp.exp(draws), dims[axis_at] // parts).reshape((-1,) + (1,) * (len(dims) - 1 - axis_at))
    return level


def centred(stream_key, shape, scale, reach, cuts=(), kind=jnp.bfloat16):
    entries = scale * jax.random.normal(stream_key, shape, jnp.float32)
    if cuts:
        entries = entries * block_scale(stream_key, shape, cuts, -0.22, 0.18)
    return jnp.clip(entries, -reach, reach).astype(kind)


def setup_inputs(seed: int = 0) -> dict:
    keys = jax.random.split(jax.random.key(seed), 6)
    return {
        "ensemble": centred(keys[0], (MEMBERS, LEV, NY, NX), 0.2, 1.1953125, ((2, 8), (3, 4))),
        "obs_cell": place_ends(jax.random.randint(keys[1], (N_GY, N_GX, OBS_DEV), 0, CY * CX), jax.random.fold_in(keys[1], 1), 0, (CY * CX) - 1).astype(jnp.int32),
        "obs_level": place_ends(jax.random.randint(keys[2], (N_GY, N_GX, OBS_DEV), 0, LEV), jax.random.fold_in(keys[2], 1), 0, LEV - 1).astype(jnp.int32),
        "innovation": centred(keys[3], (N_GY, N_GX, OBS_DEV), 1.0, 6.0, ((0, 8), (1, 4)), jnp.float32),
        "obs_weight": jnp.clip(jnp.exp(math.log(4.0) - 2.0794415 * jax.random.uniform(keys[4], (N_GY, N_GX, OBS_DEV), jnp.float32) ** block_scale(keys[4], (N_GY, N_GX, OBS_DEV), ((0, 8), (1, 4)), -0.2, 0.2)), 0.5, 4.0),
    }


KAPPA = 0.2
EPS = 1e-06

def smooth_once(field):
    padded = jnp.pad(field, ((0, 0), (0, 0), (1, 1), (1, 1)))
    beside_all = padded[:, :, 2:, 1:-1] + padded[:, :, :-2, 1:-1] + padded[:, :, 1:-1, 2:] + padded[:, :, 1:-1, :-2]
    return field + KAPPA * (beside_all - 4.0 * field)

def filtered(field):
    for sweep in range(SWEEPS):
        field = smooth_once(field)
    return field

def reference(ensemble, obs_cell, obs_level, innovation, obs_weight):
    block_row = jnp.arange(N_GY, dtype=jnp.int32)[:, None, None]
    block_col = jnp.arange(N_GX, dtype=jnp.int32)[None, :, None]
    rows = block_row * CY + obs_cell // CX
    cols = block_col * CX + obs_cell % CX
    points = (obs_level * (NY * NX) + rows * NX + cols).reshape(-1).astype(jnp.int32)
    weights = obs_weight.reshape(-1)
    members = ensemble.astype(jnp.float32)

    def adjoint_obs(values):
        state = jnp.zeros((LEV * NY * NX,), jnp.float32).at[points].add(values)
        return state.reshape(LEV, NY, NX)

    def hessian(vector):
        state = lax.optimization_barrier(jnp.sum(members * filtered(vector), axis=0))
        seen = state.reshape(-1)[points]
        back = filtered(members * adjoint_obs(weights * seen)[None])
        return (vector + back, state)
    gradient = filtered(members * adjoint_obs(weights * innovation.reshape(-1))[None])
    bnorm = jnp.sqrt(jnp.sum(gradient * gradient) + EPS)
    first = gradient / bnorm
    image_one, state_one = hessian(first)
    alpha_one = jnp.sum(first * image_one)
    remain = image_one - alpha_one * first
    beta = jnp.sqrt(jnp.sum(remain * remain) + EPS)
    second = remain / beta
    image_two, state_two = hessian(second)
    alpha_two = jnp.sum(second * image_two)
    determ = alpha_one * alpha_two - beta * beta
    coef_one = bnorm * alpha_two / determ
    coef_two = -bnorm * beta / determ
    control = coef_one * first + coef_two * second
    increment = coef_one * state_one + coef_two * state_two
    return (control, increment)
```

```python
import functools
import jax
import jax.numpy as jnp
from jax import lax
from jax.experimental import pallas as pl
from jax.experimental.pallas import tpu as pltpu
from jax.sharding import PartitionSpec as P

SWEEPS = 4
KAPPA = 0.2
EPS = 1e-06
W = 2 * SWEEPS
KEEP = 3 * W
HALF = 64


def scatter_kernel(cell_ref, level_ref, inn_ref, wt_ref, g_ref, d_ref, *, rows, cols):
    cell = cell_ref[...]
    row = level_ref[...] * rows + cell // cols
    col = cell % cols
    n = cell.shape[1]
    lr = g_ref.shape[0]
    hot = jnp.where(lax.broadcasted_iota(jnp.int32, (lr, n), 0) == row, 1.0, 0.0).astype(jnp.bfloat16)
    at = lax.broadcasted_iota(jnp.int32, (cols, n), 0) == col
    wt = wt_ref[...]
    for ref, v in ((g_ref, wt * inn_ref[...]), (d_ref, wt)):
        hi = v.astype(jnp.bfloat16).astype(jnp.float32)
        lo = v - hi
        total = None
        for part in (hi, lo):
            sel = jnp.where(at, part, 0.0).astype(jnp.bfloat16)
            term = lax.dot_general(hot, sel, (((1,), (1,)), ((), ())), preferred_element_type=jnp.float32)
            total = term if total is None else total + term
        ref[...] = total


def fill_kappa(km_ref, ks_ref, rows, cols):
    hr = km_ref.shape[0]
    gy, gx = lax.axis_index("gy"), lax.axis_index("gx")
    r = lax.broadcasted_iota(jnp.int32, (hr, cols), 0) + gy * rows - W
    rok = (r >= 0) & (r < rows * lax.axis_size("gy"))
    km_ref[...] = jnp.where(rok, KAPPA, 0.0)
    lane = lax.broadcasted_iota(jnp.int32, (hr, cols), 1) % HALF
    west = lane < KEEP
    c = jnp.where(west, lane - W, lane - HALF // 2 + cols - 2 * W) + gx * cols
    real = west | ((lane >= HALF // 2) & (lane < HALF // 2 + KEEP))
    cok = real & (c >= 0) & (c < cols * lax.axis_size("gx"))
    ks_ref[...] = jnp.where(rok & cok, KAPPA, 0.0)


def g_kernel(e_ref, s_ref, g_ref, gs_ref, p_ref, ps_ref, y_ref, km_ref, ks_ref, ym_ref, yst_ref,
             *, members, levels, rows, cols):
    hr = rows + 2 * W
    groups = members // 8
    pairs = groups // 2
    fill_kappa(km_ref, ks_ref, rows, cols)

    def e_row(l, m, r):
        return e_ref[pl.ds(((m * 8) * levels + l) * hr + r, 8, stride=levels * hr), :]

    def s_row(l, j, r):
        return s_ref[pl.ds(((l * pairs + j) * 8) * hr + r, 8, stride=hr), :]

    def sweep_all(state, vals, r):
        new = []
        for s in range(SWEEPS):
            km = km_ref[pl.ds(jnp.maximum(r - s - 1, 0), 1), :]
            ks = ks_ref[pl.ds(jnp.maximum(r - s - 1, 0), 1), :]
            out = []
            for c, u in enumerate(vals):
                q, prev = state[s][c]
                out.append((km if c < groups else ks) * (q + u))
                h = u + prev + (pltpu.roll(u, 1, 1) + pltpu.roll(u, cols - 1, 1))
                new.append((h, u))
            vals = out
        n = len(vals)
        return [new[s * n:(s + 1) * n] for s in range(SWEEPS)], vals

    count = groups + pairs
    zero = jnp.zeros((8, cols), jnp.float32)
    for l in range(levels):
        start = [[(zero, zero)] * count for _ in range(SWEEPS)]

        def first(r, state):
            gm = g_ref[l, pl.ds(r, 1), :]
            gs = gs_ref[l, pl.ds(r, 1), :]
            vals = [e_row(l, m, r) * gm for m in range(groups)] + [s_row(l, j, r) * gs for j in range(pairs)]
            state, vals = sweep_all(state, vals, r)
            o = jnp.maximum(r - SWEEPS, 0)
            for m in range(groups):
                p_ref[l * groups + m, o] = vals[m]
            for j in range(pairs):
                ps_ref[l * pairs + j, o] = vals[groups + j]
            return state

        lax.fori_loop(0, hr, first, start)

        def second(r, state):
            vals = [p_ref[l * groups + m, r] for m in range(groups)] + [ps_ref[l * pairs + j, r] for j in range(pairs)]
            state, vals = sweep_all(state, vals, r)
            o = jnp.maximum(r - SWEEPS, 0)
            acc = None
            for m in range(groups):
                t = vals[m] * e_row(l, m, o)
                acc = t if acc is None else acc + t
            ym_ref[l, o] = acc
            acc = None
            for j in range(pairs):
                t = vals[groups + j] * s_row(l, j, o)
                acc = t if acc is None else acc + t
            yst_ref[l, o] = acc
            return state

        lax.fori_loop(SWEEPS, hr - SWEEPS, second, start)
    lane = lax.broadcasted_iota(jnp.int32, (rows, cols), 1)
    for l in range(levels):
        main = jnp.sum(ym_ref[l, W:W + rows], axis=1)
        st = jnp.sum(yst_ref[l, W:W + rows], axis=1)
        st = st + pltpu.roll(st, HALF, 1)
        west = pltpu.roll(st, cols - W, 1)
        east = pltpu.roll(st, cols - W - (HALF // 2 + W), 1)
        y_ref[l] = jnp.where(lane < W, west, jnp.where(lane >= cols - W, east, main))


def g_apply(e2, s2, gm, gs, dims):
    members, levels, rows, cols = dims
    hr = rows + 2 * W
    groups = members // 8
    pairs = groups // 2
    vm = pl.BlockSpec(memory_space=pltpu.VMEM)
    f32 = jnp.float32
    return pl.pallas_call(
        functools.partial(g_kernel, members=members, levels=levels, rows=rows, cols=cols),
        out_shape=(
            jax.ShapeDtypeStruct((levels * groups, hr, 8, cols), f32),
            jax.ShapeDtypeStruct((levels * pairs, hr, 8, cols), f32),
            jax.ShapeDtypeStruct((levels, rows, cols), f32),
        ),
        in_specs=[vm] * 4,
        out_specs=(vm,) * 3,
        scratch_shapes=[pltpu.VMEM((hr, cols), f32), pltpu.VMEM((hr, cols), f32),
                        pltpu.VMEM((levels, hr, 8, cols), f32), pltpu.VMEM((levels, hr, 8, cols), f32)],
        compiler_params=pltpu.CompilerParams(vmem_limit_bytes=60000000),
    )(e2, s2, gm, gs)


def with_halo(cells, sides, width):
    for axis, dim in sides:
        count = lax.axis_size(axis)
        ends = count - 1
        head = lax.slice_in_dim(cells, 0, width, axis=dim)
        tail = lax.slice_in_dim(cells, cells.shape[dim] - width, cells.shape[dim], axis=dim)
        cells = jnp.concatenate(
            [
                lax.ppermute(tail, axis, [(i, (i + 1) % count) for i in range(ends)]),
                cells,
                lax.ppermute(head, axis, [((i + 1) % count, i) for i in range(ends)]),
            ],
            axis=dim,
        )
    return cells


def strip_of(full, cols):
    pad = jnp.zeros(full.shape[:-1] + (HALF // 2 - KEEP,), full.dtype)
    return jnp.concatenate([full[..., :KEEP], pad, full[..., full.shape[-1] - KEEP:], pad], axis=-1)


def on_device(ensemble, obs_cell, obs_level, innovation, obs_weight):
    members, levels, rows, cols = ensemble.shape
    groups = members // 8
    pairs = groups // 2
    hr = rows + 2 * W
    f32 = jnp.float32
    vm = pl.BlockSpec(memory_space=pltpu.VMEM)
    flat = lambda a: a.reshape(1, -1)
    g0, dd = pl.pallas_call(
        functools.partial(scatter_kernel, rows=rows, cols=cols),
        out_shape=(jax.ShapeDtypeStruct((levels * rows, cols), f32),) * 2,
        in_specs=[vm] * 4, out_specs=(vm, vm),
    )(flat(obs_cell), flat(obs_level), flat(innovation), flat(obs_weight))
    g0 = g0.reshape(levels, rows, cols)
    dd = dd.reshape(levels, rows, cols)
    full = with_halo(ensemble.astype(f32), (("gy", 2), ("gx", 3)), W)
    e2 = full[..., W:W + cols].reshape(members * levels * hr, cols)
    st = strip_of(full, cols)
    st = st.reshape(pairs, 2, 8, levels, hr, HALF).transpose(3, 0, 2, 4, 1, 5)
    s2 = st.reshape(levels * pairs * 8 * hr, cols)

    def apply(g):
        gf = with_halo(g, (("gy", 1), ("gx", 2)), W)
        gs = strip_of(gf, cols)
        return g_apply(e2, s2, gf[..., W:W + cols], jnp.concatenate([gs, gs], -1), ensemble.shape)

    p0, ps0, y0 = apply(g0)
    g1 = dd * y0
    p1, ps1, y1 = apply(g1)
    sums = jnp.stack([jnp.sum(g0 * y0), jnp.sum(g1 * y0), jnp.sum(g1 * y1), jnp.sum(dd * y1 * y1)])
    m = lax.psum(sums, ("gy", "gx"))
    bn2 = m[0] + EPS
    c = (EPS - m[1]) / bn2
    alpha1 = (m[0] + m[1]) / bn2
    r2 = jnp.maximum((c * c * m[0] + 2.0 * c * m[1] + m[2]) / bn2, 0.0)
    rho = (c * c * m[1] + 2.0 * c * m[2] + m[3]) / bn2
    b2 = r2 + EPS
    alpha2 = (r2 + rho) / b2
    det = alpha1 * alpha2 - b2
    ca = (alpha2 - c) / det
    cb = -1.0 / det

    pm = ca * p0[:, W:W + rows] + cb * p1[:, W:W + rows]
    ps = ca * ps0[:, W:W + rows] + cb * ps1[:, W:W + rows]
    pm = pm.reshape(levels, pairs, 2, rows, 8, cols).transpose(1, 2, 4, 0, 3, 5).reshape(members, levels, rows, cols)
    ps = ps.reshape(levels, pairs, rows, 8, 2, HALF).transpose(1, 4, 3, 0, 2, 5).reshape(members, levels, rows, HALF)
    control = jnp.concatenate([ps[..., W:2 * W], pm[..., W:cols - W], ps[..., HALF // 2 + W:HALF // 2 + 2 * W]], -1)
    increment = ca * y0 + cb * y1
    return (control, increment)


def solution(mesh):
    return jax.shard_map(
        on_device,
        mesh=mesh,
        in_specs=(
            P(None, None, "gy", "gx"),
            P("gy", "gx", None),
            P("gy", "gx", None),
            P("gy", "gx", None),
            P("gy", "gx", None),
        ),
        out_specs=(P(None, None, "gy", "gx"), P(None, "gy", "gx")),
        check_vma=False,
    )
```

```python
import functools
import math
import jax
import jax.numpy as jnp
from jax import lax
from jax.experimental import pallas as pl
from jax.experimental.pallas import tpu as pltpu
from jax.sharding import PartitionSpec as P

SWEEPS = 4
KAPPA = 0.2
EPS = 1e-06
W = 2 * SWEEPS
KEEP = 3 * W
HALF = 64
UNROLL = 4


def scatter_kernel(cell_ref, level_ref, inn_ref, wt_ref, g_ref, d_ref, *, rows, cols):
    cell = cell_ref[...]
    row = level_ref[...] * rows + cell // cols
    col = cell % cols
    n = cell.shape[1]
    lr = g_ref.shape[0]
    hot = jnp.where(lax.broadcasted_iota(jnp.int32, (lr, n), 0) == row, 1.0, 0.0).astype(jnp.bfloat16)
    at = lax.broadcasted_iota(jnp.int32, (cols, n), 0) == col
    wt = wt_ref[...]
    for ref, v in ((g_ref, wt * inn_ref[...]), (d_ref, wt)):
        hi = v.astype(jnp.bfloat16).astype(jnp.float32)
        lo = v - hi
        total = None
        for part in (hi, lo):
            sel = jnp.where(at, part, 0.0).astype(jnp.bfloat16)
            term = lax.dot_general(hot, sel, (((1,), (1,)), ((), ())), preferred_element_type=jnp.float32)
            total = term if total is None else total + term
        ref[...] = total


def weight_kernel(wm_ref, ws_ref, *, cols):
    i = lax.broadcasted_iota(jnp.int32, (cols, cols), 0)
    j = lax.broadcasted_iota(jnp.int32, (cols, cols), 1)
    near = jnp.abs(i - j) <= 1
    gx = lax.axis_index("gx")

    def real(lane):
        lane = lane % HALF
        west = lane < KEEP
        c = jnp.where(west, lane - W, lane - HALF // 2 + cols - 2 * W) + gx * cols
        inside = west | ((lane >= HALF // 2) & (lane < HALF // 2 + KEEP))
        return inside & (c >= 0) & (c < cols * lax.axis_size("gx"))

    for ref, ok in ((wm_ref, near), (ws_ref, near & real(i) & real(j))):
        one = jnp.where(ok, 1.0, 0.0).astype(jnp.bfloat16)
        power = one
        for s in range(1, SWEEPS + 1):
            if s > 1:
                power = jnp.dot(power, one, preferred_element_type=jnp.float32).astype(jnp.bfloat16)
            scaled = (power.astype(jnp.float32) * float(math.comb(SWEEPS, s))).astype(jnp.bfloat16)
            ref[0:cols, (s - 1) * cols:s * cols] = scaled
            ref[cols:2 * cols, (s - 1) * cols:s * cols] = scaled


def g_kernel(e_ref, s_ref, g_ref, gs_ref, d_ref, wm_ref, ws_ref, p_ref, ps_ref, y_ref, km_ref, ym_ref, yst_ref,
             u_ref, lhs_ref, f_ref, *, members, levels, rows, cols):
    hr = rows + 2 * W
    groups = members // 8
    pairs = groups // 2
    count = groups + pairs
    scale = KAPPA ** SWEEPS
    gy = lax.axis_index("gy")
    rr = lax.broadcasted_iota(jnp.int32, (hr, cols), 0) + gy * rows - W
    km_ref[...] = jnp.where((rr >= 0) & (rr < rows * lax.axis_size("gy")), 1.0, 0.0)

    def e_row(l, m, r):
        return e_ref[pl.ds(((m * 8) * levels + l) * hr + r, 8, stride=levels * hr), :]

    def s_row(l, j, r):
        return s_ref[pl.ds(((l * pairs + j) * 8) * hr + r, 8, stride=hr), :]

    def ek_row(l, c, r):
        return e_row(l, c, r) if c < groups else s_row(l, c - groups, r)

    def split(c, r, u):
        hi = u.astype(jnp.bfloat16)
        lo = (u - hi.astype(jnp.float32)).astype(jnp.bfloat16)
        return hi, lo

    def products(lo_row, n):
        for c in range(count):
            w = wm_ref if c < groups else ws_ref
            f_ref[c, pl.ds(lo_row * 8, n * 8), :] = jnp.dot(
                lhs_ref[c, pl.ds(lo_row * 8, n * 8), :], w[...], preferred_element_type=jnp.float32)

    def sweep_all(state, vals, r):
        new = []
        for s in range(SWEEPS):
            o = jnp.maximum(r - s - 1, 0)
            km = km_ref[pl.ds(o, 1), :]
            out = []
            at = pl.ds(pl.multiple_of(o * 8, 8), 8)
            for c, u in enumerate(vals):
                older, prev = state[s][c]
                out.append(km * (older + u) + f_ref[c, at, s * cols:(s + 1) * cols])
                new.append((prev, u))
            vals = out
        return [new[s * count:(s + 1) * count] for s in range(SWEEPS)], [v * scale for v in vals]

    zero = km_ref[0:8, :] * 0.0
    start = [[(zero, zero)] * count for _ in range(SWEEPS)]
    step = 16

    def store_lhs(c, r, us):
        his, los = zip(*[split(c, r, u) for u in us])
        at = pl.ds(pl.multiple_of(r * 8, 16), 16)
        lhs_ref[c, at, 0:cols] = jnp.concatenate(his, axis=0)
        lhs_ref[c, at, cols:2 * cols] = jnp.concatenate(los, axis=0)

    for l in range(levels):
        def fill(i, carry):
            r = i * 2
            for c in range(count):
                us = []
                for k in range(2):
                    g = (g_ref if c < groups else gs_ref)[l, pl.ds(r + k, 1), :]
                    u = ek_row(l, c, r + k) * g
                    u_ref[c, r + k] = u
                    us.append(u)
                store_lhs(c, r, us)
            return carry

        lax.fori_loop(0, hr // 2, fill, 0, unroll=2)
        lax.fori_loop(0, hr // step, lambda i, x: (products(pl.multiple_of(i * step, step), step), x)[1], 0)

        def first(r, state):
            state, vals = sweep_all(state, [u_ref[c, r] for c in range(count)], r)
            o = jnp.maximum(r - SWEEPS, 0)
            for m in range(groups):
                p_ref[l * groups + m, o] = vals[m]
            for j in range(pairs):
                ps_ref[l * pairs + j, o] = vals[groups + j]
            return state

        lax.fori_loop(0, hr, first, start, unroll=UNROLL)

        def refill(i, carry):
            r = i * 2
            for c in range(count):
                p = p_ref.at[l * groups + c] if c < groups else ps_ref.at[l * pairs + c - groups]
                store_lhs(c, r, [p[r], p[r + 1]])
            return carry

        lax.fori_loop(SWEEPS // 2, (hr - SWEEPS) // 2, refill, 0, unroll=2)
        lax.fori_loop(0, hr // step, lambda i, x: (products(pl.multiple_of(i * step, step), step), x)[1], 0)

        def second(r, state):
            vals = [p_ref[l * groups + m, r] for m in range(groups)] + [ps_ref[l * pairs + j, r] for j in range(pairs)]
            state, vals = sweep_all(state, vals, r)
            o = jnp.maximum(r - SWEEPS, 0)
            acc = None
            for m in range(groups):
                t = vals[m] * e_row(l, m, o)
                acc = t if acc is None else acc + t
            ym_ref[l, o] = acc
            acc = None
            for j in range(pairs):
                t = vals[groups + j] * s_row(l, j, o)
                acc = t if acc is None else acc + t
            yst_ref[l, o] = acc
            return state

        lax.fori_loop(SWEEPS, hr - SWEEPS, second, start, unroll=UNROLL)
    lane = lax.broadcasted_iota(jnp.int32, (rows, cols), 1)
    for l in range(levels):
        main = jnp.sum(ym_ref[l, W:W + rows], axis=1)
        st = jnp.sum(yst_ref[l, W:W + rows], axis=1)
        st = st + pltpu.roll(st, HALF, 1)
        west = pltpu.roll(st, cols - W, 1)
        east = pltpu.roll(st, cols - W - (HALF // 2 + W), 1)
        y_ref[l] = jnp.where(lane < W, west, jnp.where(lane >= cols - W, east, main))


def g_apply(e2, s2, gm, gs, dd, wm, ws, dims):
    members, levels, rows, cols = dims
    hr = rows + 2 * W
    groups = members // 8
    pairs = groups // 2
    count = groups + pairs
    vm = pl.BlockSpec(memory_space=pltpu.VMEM)
    f32 = jnp.float32
    return pl.pallas_call(
        functools.partial(g_kernel, members=members, levels=levels, rows=rows, cols=cols),
        out_shape=(
            jax.ShapeDtypeStruct((levels * groups, hr, 8, cols), f32),
            jax.ShapeDtypeStruct((levels * pairs, hr, 8, cols), f32),
            jax.ShapeDtypeStruct((levels, rows, cols), f32),
        ),
        in_specs=[vm] * 7,
        out_specs=(vm,) * 3,
        scratch_shapes=[pltpu.VMEM((hr, cols), f32),
                        pltpu.VMEM((levels, hr, 8, cols), f32), pltpu.VMEM((levels, hr, 8, cols), f32),
                        pltpu.VMEM((count, hr, 8, cols), f32),
                        pltpu.VMEM((count, hr * 8, 2 * cols), jnp.bfloat16),
                        pltpu.VMEM((count, hr * 8, SWEEPS * cols), f32)],
        compiler_params=pltpu.CompilerParams(vmem_limit_bytes=60000000),
    )(e2, s2, gm, gs, dd, wm, ws)


def sum_kernel(x_ref, o_ref, mid_ref, ra_ref, rb_ref, sa, qa, sb, qb):
    nx, ny = lax.axis_size("gx"), lax.axis_size("gy")
    mx, my = lax.axis_index("gx"), lax.axis_index("gy")
    bar = pltpu.get_barrier_semaphore()
    for axis, n, me in (("gx", nx, mx), ("gy", ny, my)):
        for k in range(1, n):
            pl.semaphore_signal(bar, inc=1, device_id={axis: lax.rem(me + k, n)}, device_id_type=pl.DeviceIdType.MESH)
    pl.semaphore_wait(bar, nx + ny - 2)

    def stage(axis, n, me, src, land, ssem, rsem):
        copies = []
        for k in range(1, n):
            copies.append(pltpu.make_async_remote_copy(
                src_ref=src, dst_ref=land.at[k - 1], send_sem=ssem.at[k - 1], recv_sem=rsem.at[k - 1],
                device_id={axis: lax.rem(me + k, n)}, device_id_type=pl.DeviceIdType.MESH))
            copies[-1].start()
        for c in copies:
            c.wait_recv()
        total = src[...]
        for k in range(n - 1):
            total = total + land[k]
        return copies, total

    ca, total = stage("gx", nx, mx, x_ref, ra_ref, sa, qa)
    mid_ref[...] = total
    cb, total = stage("gy", ny, my, mid_ref, rb_ref, sb, qb)
    o_ref[...] = total
    for c in ca + cb:
        c.wait_send()


def sum_all(x):
    nx, ny = lax.axis_size("gx"), lax.axis_size("gy")
    vm = pl.BlockSpec(memory_space=pltpu.VMEM)
    dma = pltpu.SemaphoreType.DMA
    return pl.pallas_call(
        sum_kernel,
        out_shape=jax.ShapeDtypeStruct(x.shape, x.dtype),
        in_specs=[vm],
        out_specs=vm,
        scratch_shapes=[pltpu.VMEM(x.shape, x.dtype), pltpu.VMEM((nx - 1,) + x.shape, x.dtype),
                        pltpu.VMEM((ny - 1,) + x.shape, x.dtype),
                        dma((nx - 1,)), dma((nx - 1,)), dma((ny - 1,)), dma((ny - 1,))],
        compiler_params=pltpu.CompilerParams(collective_id=0, has_side_effects=True),
    )(x)


def with_halo(cells, sides, width):
    for axis, dim in sides:
        count = lax.axis_size(axis)
        ends = count - 1
        head = lax.slice_in_dim(cells, 0, width, axis=dim)
        tail = lax.slice_in_dim(cells, cells.shape[dim] - width, cells.shape[dim], axis=dim)
        cells = jnp.concatenate(
            [
                lax.ppermute(tail, axis, [(i, (i + 1) % count) for i in range(ends)]),
                cells,
                lax.ppermute(head, axis, [((i + 1) % count, i) for i in range(ends)]),
            ],
            axis=dim,
        )
    return cells


def strip_of(full, cols):
    pad = jnp.zeros(full.shape[:-1] + (HALF // 2 - KEEP,), full.dtype)
    return jnp.concatenate([full[..., :KEEP], pad, full[..., full.shape[-1] - KEEP:], pad], axis=-1)


def on_device(ensemble, obs_cell, obs_level, innovation, obs_weight):
    members, levels, rows, cols = ensemble.shape
    groups = members // 8
    pairs = groups // 2
    hr = rows + 2 * W
    f32 = jnp.float32
    vm = pl.BlockSpec(memory_space=pltpu.VMEM)
    flat = lambda a: a.reshape(1, -1)
    g0, dd = pl.pallas_call(
        functools.partial(scatter_kernel, rows=rows, cols=cols),
        out_shape=(jax.ShapeDtypeStruct((levels * rows, cols), f32),) * 2,
        in_specs=[vm] * 4, out_specs=(vm, vm),
    )(flat(obs_cell), flat(obs_level), flat(innovation), flat(obs_weight))
    g0 = g0.reshape(levels, rows, cols)
    dd = dd.reshape(levels, rows, cols)
    wm, ws = pl.pallas_call(
        functools.partial(weight_kernel, cols=cols),
        out_shape=(jax.ShapeDtypeStruct((2 * cols, SWEEPS * cols), jnp.bfloat16),) * 2,
        out_specs=(vm, vm),
    )()
    full = with_halo(ensemble.astype(f32), (("gy", 2), ("gx", 3)), W)
    e2 = full[..., W:W + cols].reshape(members * levels * hr, cols)
    st = strip_of(full, cols)
    st = st.reshape(pairs, 2, 8, levels, hr, HALF).transpose(3, 0, 2, 4, 1, 5)
    s2 = st.reshape(levels * pairs * 8 * hr, cols)

    def apply(g):
        gf = with_halo(g, (("gy", 1), ("gx", 2)), W)
        gs = strip_of(gf, cols)
        return g_apply(e2, s2, gf[..., W:W + cols], jnp.concatenate([gs, gs], -1), dd, wm, ws, ensemble.shape)

    p0, ps0, y0 = apply(g0)
    g1 = dd * y0
    p1, ps1, y1 = apply(g1)
    sums = jnp.stack([jnp.sum(v, axis=(0, 1)) for v in (g0 * y0, g1 * y0, g1 * y1, dd * y1 * y1)])
    m = jnp.sum(sum_all(jnp.concatenate([sums, jnp.zeros_like(sums)])), axis=1)
    bn2 = m[0] + EPS
    c = (EPS - m[1]) / bn2
    alpha1 = (m[0] + m[1]) / bn2
    r2 = jnp.maximum((c * c * m[0] + 2.0 * c * m[1] + m[2]) / bn2, 0.0)
    rho = (c * c * m[1] + 2.0 * c * m[2] + m[3]) / bn2
    b2 = r2 + EPS
    alpha2 = (r2 + rho) / b2
    det = alpha1 * alpha2 - b2
    ca = (alpha2 - c) / det
    cb = -1.0 / det

    pm = ca * p0[:, W:W + rows] + cb * p1[:, W:W + rows]
    ps = ca * ps0[:, W:W + rows] + cb * ps1[:, W:W + rows]
    pm = pm.reshape(levels, pairs, 2, rows, 8, cols).transpose(1, 2, 4, 0, 3, 5).reshape(members, levels, rows, cols)
    ps = ps.reshape(levels, pairs, rows, 8, 2, HALF).transpose(1, 4, 3, 0, 2, 5).reshape(members, levels, rows, HALF)
    control = jnp.concatenate([ps[..., W:2 * W], pm[..., W:cols - W], ps[..., HALF // 2 + W:HALF // 2 + 2 * W]], -1)
    increment = ca * y0 + cb * y1
    return (control, increment)


def solution(mesh):
    return jax.shard_map(
        on_device,
        mesh=mesh,
        in_specs=(
            P(None, None, "gy", "gx"),
            P("gy", "gx", None),
            P("gy", "gx", None),
            P("gy", "gx", None),
            P("gy", "gx", None),
        ),
        out_specs=(P(None, None, "gy", "gx"), P(None, "gy", "gx")),
        check_vma=False,
    )
```

```python
import functools
import math
import jax
import jax.numpy as jnp
from jax import lax
from jax.experimental import pallas as pl
from jax.experimental.pallas import tpu as pltpu
from jax.sharding import PartitionSpec as P

SWEEPS = 4
KAPPA = 0.2
EPS = 1e-06
W = 2 * SWEEPS
HALF = 64
UNROLL = 4


def scatter(cell_ref, level_ref, inn_ref, wt_ref, g_ref, d_ref):
    levels, rows, cols = g_ref.shape
    cell = cell_ref[...]
    row = level_ref[...] * rows + cell // cols
    col = cell % cols
    n = cell.shape[1]
    hot = jnp.where(lax.broadcasted_iota(jnp.int32, (levels * rows, n), 0) == row, 1.0, 0.0).astype(jnp.bfloat16)
    at = lax.broadcasted_iota(jnp.int32, (cols, n), 0) == col
    wt = wt_ref[...]
    for ref, v in ((g_ref, wt * inn_ref[...]), (d_ref, wt)):
        hi = v.astype(jnp.bfloat16).astype(jnp.float32)
        lo = v - hi
        total = None
        for part in (hi, lo):
            sel = jnp.where(at, part, 0.0).astype(jnp.bfloat16)
            term = lax.dot_general(hot, sel, (((1,), (1,)), ((), ())), preferred_element_type=jnp.float32)
            total = term if total is None else total + term
        for l in range(levels):
            ref[l] = total[l * rows:(l + 1) * rows]


SIDES = [(-1, 0), (1, 0), (0, -1), (0, 1), (-1, -1), (-1, 1), (1, -1), (1, 1)]


def peer(dy, dx):
    ny, nx = lax.axis_size("gy"), lax.axis_size("gx")
    return {"gy": lax.rem(lax.axis_index("gy") + dy + ny, ny), "gx": lax.rem(lax.axis_index("gx") + dx + nx, nx)}


def meet():
    bar = pltpu.get_barrier_semaphore()
    for dy, dx in SIDES:
        pl.semaphore_signal(bar, inc=1, device_id=peer(dy, dx), device_id_type=pl.DeviceIdType.MESH)
    pl.semaphore_wait(bar, len(SIDES))


def send_all(pairs, ssem, rsem):
    copies = []
    for n, ((dy, dx), (src, dst)) in enumerate(zip(SIDES, pairs)):
        copies.append(pltpu.make_async_remote_copy(
            src_ref=src, dst_ref=dst, send_sem=ssem.at[n], recv_sem=rsem.at[n],
            device_id=peer(dy, dx), device_id_type=pl.DeviceIdType.MESH))
        copies[-1].start()
    return copies


def pack_state(g_ref, pe_ref, pw_ref):
    levels, rows, cols = g_ref.shape
    block = lax.broadcasted_iota(jnp.int32, (8, cols), 1) // W
    e = w = jnp.zeros((8, cols), jnp.float32)
    per = rows // 8
    for l in range(levels):
        for t in range(per):
            p = l * per + t
            x = pltpu.roll(g_ref[l, t * 8:t * 8 + 8], (p * W + W) % cols, 1)
            e = jnp.where(block == p, x, e)
            w = jnp.where(block == (p + 1) % (cols // W), x, w)
    pe_ref[...] = e
    pw_ref[...] = w


def unpack_state(g_ref, land_n, land_p, gm_ref, gs_ref):
    levels, rows, cols = g_ref.shape
    hr = rows + 2 * W
    per = rows // 8
    lane = lax.broadcasted_iota(jnp.int32, (8, cols), 1)
    block = lane // W
    gy, gx = lax.axis_index("gy"), lax.axis_index("gx")
    c = strip_col(lane, cols) + gx * cols
    cok = (lane % HALF < 6 * W) & (c >= 0) & (c < cols * lax.axis_size("gx"))
    for l in range(levels):
        for t in range(-1, per + 1):
            if t < 0:
                x, pe, pw, p = land_n[1, l], land_p[5], land_p[4], l * per + per - 1
            elif t == per:
                x, pe, pw, p = land_n[0, l], land_p[3], land_p[2], l * per
            else:
                x, pe, pw, p = g_ref[l, t * 8:t * 8 + 8], land_p[1], land_p[0], l * per + t
            r = lax.broadcasted_iota(jnp.int32, (8, cols), 0) + gy * rows + t * 8
            rok = (r >= 0) & (r < rows * lax.axis_size("gy"))
            x = jnp.where(rok, x, 0.0)
            z = jnp.where(block == p, pe, pw)
            z1 = pltpu.roll(z, (cols - p * W) % cols, 1)
            z2 = pltpu.roll(z, (cols - p * W + HALF) % cols, 1)
            own = jnp.where(lane < HALF, pltpu.roll(x, 4 * W, 1), pltpu.roll(x, HALF + 4 * W, 1))
            halo = jnp.where(lane < HALF, z1, z2)
            gs = jnp.where(lane % HALF < 2 * W, halo, own)
            at = slice((t + 1) * 8, (t + 2) * 8)
            gm_ref[l, at] = x
            gs_ref[l, at] = jnp.where(rok & cok, gs, 0.0)


def state_pairs(g_ref, pe_ref, pw_ref, land_n, land_p):
    rows = g_ref.shape[1]
    return [(g_ref.at[:, 0:W], land_n.at[0]), (g_ref.at[:, rows - W:rows], land_n.at[1])] + [
        (pw_ref if dx < 0 else pe_ref, land_p.at[n]) for n, (dy, dx) in enumerate(SIDES[2:])]


def state_scratch(levels, cols):
    f32 = jnp.float32
    dma = pltpu.SemaphoreType.DMA
    return [pltpu.VMEM((8, cols), f32), pltpu.VMEM((8, cols), f32), pltpu.VMEM((2, levels, W, cols), f32),
            pltpu.VMEM((6, 8, cols), f32), dma((8,)), dma((8,))]


def prep_kernel(ens_ref, cell_ref, level_ref, inn_ref, wt_ref, e_ref, s_ref, g_ref, d_ref, gm_ref, gs_ref,
                ec_ref, pe_ref, pw_ref, en_ref, pee_ref, pew_ref, pc_ref, es, er,
                gpe, gpw, gn, gp, ss, sr):
    members, levels, rows, cols = ens_ref.shape
    hr = rows + 2 * W
    per = rows // 8
    pairs = members // 16
    lane = lax.broadcasted_iota(jnp.int32, (8, cols), 1)
    block = lane // W
    nb = cols // W

    def convert(k, x):
        for l in range(levels):
            ec_ref[k * levels + l] = ens_ref[k, l].astype(jnp.float32)
        return x

    lax.fori_loop(0, members, convert, 0)

    def pack(t, x):
        at = pl.ds(pl.multiple_of(t * 8, 8), 8)
        for l in range(levels):
            for j in range(pairs):
                e = w = jnp.zeros((8, cols), jnp.float32)
                for b in range(2):
                    for i in range(8):
                        p = b * 8 + i
                        x8 = pltpu.roll(ec_ref[(16 * j + p) * levels + l, at, :], (p * W + W) % cols, 1)
                        e = jnp.where(block == p, x8, e)
                        w = jnp.where(block == (p + 1) % nb, x8, w)
                pe_ref[l * pairs + j, at, :] = e
                pw_ref[l * pairs + j, at, :] = w
        return x

    lax.fori_loop(0, per, pack, 0)
    meet()
    top, bottom = slice(0, W), slice(rows - W, rows)
    jobs = [(ec_ref.at[:, top], en_ref.at[0]), (ec_ref.at[:, bottom], en_ref.at[1]), (pw_ref, pew_ref), (pe_ref, pee_ref)]
    for n, (dy, dx) in enumerate(SIDES[4:]):
        src = pw_ref if dx < 0 else pe_ref
        jobs.append((src.at[:, top if dy < 0 else bottom], pc_ref.at[n]))
    ecopies = send_all(jobs, es, er)
    scatter(cell_ref, level_ref, inn_ref, wt_ref, g_ref, d_ref)
    pack_state(g_ref, gpe, gpw)
    gcopies = send_all(state_pairs(g_ref, gpe, gpw, gn, gp), ss, sr)

    def center(f, x):
        e_ref[pl.ds(pl.multiple_of(f * hr + W, 8), rows), :] = ec_ref[f]
        return x

    lax.fori_loop(0, members * levels, center, 0)
    for c in ecopies:
        c.wait_recv()

    def edges(f, x):
        e_ref[pl.ds(pl.multiple_of(f * hr, 8), W), :] = en_ref[1, f]
        e_ref[pl.ds(pl.multiple_of(f * hr + W + rows, 8), W), :] = en_ref[0, f]
        return x

    lax.fori_loop(0, members * levels, edges, 0)

    def strip_tile(lj, i, l, j, row, pe, pw):
        a = e_ref[pl.ds(pl.multiple_of(((16 * j + i) * levels + l) * hr + row, 8), 8), :]
        b = e_ref[pl.ds(pl.multiple_of(((16 * j + 8 + i) * levels + l) * hr + row, 8), 8), :]
        own = jnp.where(lane < HALF, pltpu.roll(a, 4 * W, 1), pltpu.roll(b, HALF + 4 * W, 1))
        z = pltpu.roll(jnp.where(block % 8 == i, pe, pw), (cols - i * W) % cols, 1)
        s_ref[pl.ds(pl.multiple_of((lj * 8 + i) * hr + row, 8), 8), :] = jnp.where(lane % HALF < 2 * W, z, own)

    for l in range(levels):
        for j in range(pairs):
            lj = l * pairs + j

            def mid(t, x):
                at = pl.ds(pl.multiple_of(t * 8, 8), 8)
                pe, pw = pee_ref[lj, at, :], pew_ref[lj, at, :]
                for i in range(8):
                    strip_tile(lj, i, l, j, W + t * 8, pe, pw)
                return x

            lax.fori_loop(0, per, mid, 0)
            for i in range(8):
                strip_tile(lj, i, l, j, 0, pc_ref[3, lj], pc_ref[2, lj])
                strip_tile(lj, i, l, j, W + rows, pc_ref[1, lj], pc_ref[0, lj])
    for c in gcopies:
        c.wait_recv()
    unpack_state(g_ref, gn, gp, gm_ref, gs_ref)
    for c in ecopies + gcopies:
        c.wait_send()


def prep(ensemble, cell, level, inn, wt):
    members, levels, rows, cols = ensemble.shape
    hr = rows + 2 * W
    f = members * levels
    q = levels * (members // 16)
    f32 = jnp.float32
    vm = pl.BlockSpec(memory_space=pltpu.VMEM)
    dma = pltpu.SemaphoreType.DMA
    sds = lambda *s: jax.ShapeDtypeStruct(s, f32)
    return pl.pallas_call(
        prep_kernel,
        out_shape=(sds(f * hr, cols), sds(q * 8 * hr, cols), sds(levels, rows, cols), sds(levels, rows, cols),
                   sds(levels, hr, cols), sds(levels, hr, cols)),
        in_specs=[vm] * 5,
        out_specs=(vm,) * 6,
        scratch_shapes=[pltpu.VMEM((f, rows, cols), f32), pltpu.VMEM((q, rows, cols), f32), pltpu.VMEM((q, rows, cols), f32),
                        pltpu.VMEM((2, f, W, cols), f32), pltpu.VMEM((q, rows, cols), f32), pltpu.VMEM((q, rows, cols), f32),
                        pltpu.VMEM((4, q, W, cols), f32), dma((8,)), dma((8,))] + state_scratch(levels, cols),
        compiler_params=pltpu.CompilerParams(collective_id=1, has_side_effects=True, vmem_limit_bytes=60000000),
    )(ensemble, cell, level, inn, wt)


def next_kernel(y_ref, d_ref, gm_ref, gs_ref, g_ref, gpe, gpw, gn, gp, ss, sr):
    g_ref[...] = d_ref[...] * y_ref[...]
    pack_state(g_ref, gpe, gpw)
    meet()
    copies = send_all(state_pairs(g_ref, gpe, gpw, gn, gp), ss, sr)
    for c in copies:
        c.wait_recv()
    unpack_state(g_ref, gn, gp, gm_ref, gs_ref)
    for c in copies:
        c.wait_send()


def next_state(y, d):
    levels, rows, cols = y.shape
    vm = pl.BlockSpec(memory_space=pltpu.VMEM)
    return pl.pallas_call(
        next_kernel,
        out_shape=(jax.ShapeDtypeStruct((levels, rows + 2 * W, cols), jnp.float32),) * 2,
        in_specs=[vm] * 2,
        out_specs=(vm,) * 2,
        scratch_shapes=[pltpu.VMEM((levels, rows, cols), jnp.float32)] + state_scratch(levels, cols),
        compiler_params=pltpu.CompilerParams(collective_id=2, has_side_effects=True),
    )(y, d)


def out_kernel(m_ref, p0_ref, s0_ref, p1_ref, s1_ref, y0_ref, y1_ref, c_ref, inc_ref):
    levels, rows, cols = y0_ref.shape
    groups = p0_ref.shape[0] // levels
    pairs = groups // 2
    m = jnp.sum(m_ref[...], axis=1, keepdims=True)
    m = [m[k:k + 1] for k in range(4)]
    bn2 = m[0] + EPS
    c = (EPS - m[1]) / bn2
    alpha1 = (m[0] + m[1]) / bn2
    r2 = jnp.maximum((c * c * m[0] + 2.0 * c * m[1] + m[2]) / bn2, 0.0)
    rho = (c * c * m[1] + 2.0 * c * m[2] + m[3]) / bn2
    b2 = r2 + EPS
    alpha2 = (r2 + rho) / b2
    det = alpha1 * alpha2 - b2
    ca = jnp.broadcast_to((alpha2 - c) / det, (8, cols))
    cb = jnp.broadcast_to(-1.0 / det, (8, cols))
    for l in range(levels):
        for t in range(rows // 8):
            at = slice(t * 8, t * 8 + 8)
            inc_ref[l, at] = ca * y0_ref[l, at] + cb * y1_ref[l, at]
    lane = lax.broadcasted_iota(jnp.int32, (8, cols), 1)
    edge = (lane < W) | (lane >= cols - W)
    for l in range(levels):
        for j in range(pairs):
            def row(r, x):
                s = ca * s0_ref[l * pairs + j, W + r] + cb * s1_ref[l * pairs + j, W + r]
                for b in range(2):
                    g = l * groups + 2 * j + b
                    main = ca * p0_ref[g, W + r] + cb * p1_ref[g, W + r]
                    v = jnp.where(edge, pltpu.roll(s, (2 * cols - 4 * W - b * HALF) % cols, 1), main)
                    c_ref[pl.ds(((2 * j + b) * 8 * levels + l) * rows + r, 8, stride=levels * rows), :] = v
                return x

            lax.fori_loop(0, rows, row, 0, unroll=8)


def strip_col(lane, cols):
    lane = lane % HALF
    return jnp.where(lane < W, lane - W, jnp.where(lane < 2 * W, lane - W + cols,
                     jnp.where(lane < 4 * W, lane - 4 * W + cols, lane - 4 * W)))


def weight_kernel(wm_ref, ws_ref, *, cols):
    i = lax.broadcasted_iota(jnp.int32, (cols, cols), 0)
    j = lax.broadcasted_iota(jnp.int32, (cols, cols), 1)
    near = jnp.abs(i - j) <= 1
    gx = lax.axis_index("gx")

    def real(lane):
        c = strip_col(lane, cols) + gx * cols
        return (lane % HALF < 6 * W) & (c >= 0) & (c < cols * lax.axis_size("gx"))

    si, sj = strip_col(i, cols), strip_col(j, cols)
    same = ((i < HALF) == (j < HALF)) & (jnp.abs(si - sj) <= 1)

    for ref, ok in ((wm_ref, near), (ws_ref, same & real(i) & real(j))):
        one = jnp.where(ok, 1.0, 0.0).astype(jnp.bfloat16)
        power = one
        for s in range(1, SWEEPS + 1):
            if s > 1:
                power = jnp.dot(power, one, preferred_element_type=jnp.float32).astype(jnp.bfloat16)
            scaled = (power.astype(jnp.float32) * float(math.comb(SWEEPS, s))).astype(jnp.bfloat16)
            ref[0:cols, (s - 1) * cols:s * cols] = scaled
            ref[cols:2 * cols, (s - 1) * cols:s * cols] = scaled


def g_kernel(e_ref, s_ref, g_ref, gs_ref, wm_ref, ws_ref, p_ref, ps_ref, y_ref, km_ref, ym_ref, yst_ref,
             u_ref, lhs_ref, f_ref, *, members, levels, rows, cols):
    hr = rows + 2 * W
    groups = members // 8
    pairs = groups // 2
    count = groups + pairs
    scale = KAPPA ** SWEEPS
    gy = lax.axis_index("gy")
    rr = lax.broadcasted_iota(jnp.int32, (hr, cols), 0) + gy * rows - W
    km_ref[...] = jnp.where((rr >= 0) & (rr < rows * lax.axis_size("gy")), 1.0, 0.0)

    def e_row(l, m, r):
        return e_ref[pl.ds(((m * 8) * levels + l) * hr + r, 8, stride=levels * hr), :]

    def s_row(l, j, r):
        return s_ref[pl.ds(((l * pairs + j) * 8) * hr + r, 8, stride=hr), :]

    def ek_row(l, c, r):
        return e_row(l, c, r) if c < groups else s_row(l, c - groups, r)

    def split(c, r, u):
        hi = u.astype(jnp.bfloat16)
        lo = (u - hi.astype(jnp.float32)).astype(jnp.bfloat16)
        return hi, lo

    def products(lo_row, n):
        for c in range(count):
            w = wm_ref if c < groups else ws_ref
            f_ref[c, pl.ds(lo_row * 8, n * 8), :] = jnp.dot(
                lhs_ref[c, pl.ds(lo_row * 8, n * 8), :], w[...], preferred_element_type=jnp.float32)

    def sweep_all(state, vals, r):
        new = []
        for s in range(SWEEPS):
            o = jnp.maximum(r - s - 1, 0)
            km = km_ref[pl.ds(o, 1), :]
            out = []
            at = pl.ds(pl.multiple_of(o * 8, 8), 8)
            for c, u in enumerate(vals):
                older, prev = state[s][c]
                out.append(km * (older + u) + f_ref[c, at, s * cols:(s + 1) * cols])
                new.append((prev, u))
            vals = out
        return [new[s * count:(s + 1) * count] for s in range(SWEEPS)], [v * scale for v in vals]

    zero = km_ref[0:8, :] * 0.0
    start = [[(zero, zero)] * count for _ in range(SWEEPS)]
    step = 16

    def store_lhs(c, r, us):
        his, los = zip(*[split(c, r, u) for u in us])
        at = pl.ds(pl.multiple_of(r * 8, 16), 16)
        lhs_ref[c, at, 0:cols] = jnp.concatenate(his, axis=0)
        lhs_ref[c, at, cols:2 * cols] = jnp.concatenate(los, axis=0)

    for l in range(levels):
        def fill(i, carry):
            r = i * 2
            for c in range(count):
                us = []
                for k in range(2):
                    g = (g_ref if c < groups else gs_ref)[l, pl.ds(r + k, 1), :]
                    u = ek_row(l, c, r + k) * g
                    u_ref[c, r + k] = u
                    us.append(u)
                store_lhs(c, r, us)
            return carry

        lax.fori_loop(0, hr // 2, fill, 0, unroll=2)
        lax.fori_loop(0, hr // step, lambda i, x: (products(pl.multiple_of(i * step, step), step), x)[1], 0)

        def first(r, state):
            state, vals = sweep_all(state, [u_ref[c, r] for c in range(count)], r)
            o = jnp.maximum(r - SWEEPS, 0)
            for m in range(groups):
                p_ref[l * groups + m, o] = vals[m]
            for j in range(pairs):
                ps_ref[l * pairs + j, o] = vals[groups + j]
            return state

        lax.fori_loop(0, hr, first, start, unroll=UNROLL)

        def refill(i, carry):
            r = i * 2
            for c in range(count):
                p = p_ref.at[l * groups + c] if c < groups else ps_ref.at[l * pairs + c - groups]
                store_lhs(c, r, [p[r], p[r + 1]])
            return carry

        lax.fori_loop(SWEEPS // 2, (hr - SWEEPS) // 2, refill, 0, unroll=2)
        lax.fori_loop(0, hr // step, lambda i, x: (products(pl.multiple_of(i * step, step), step), x)[1], 0)

        def second(r, state):
            vals = [p_ref[l * groups + m, r] for m in range(groups)] + [ps_ref[l * pairs + j, r] for j in range(pairs)]
            state, vals = sweep_all(state, vals, r)
            o = jnp.maximum(r - SWEEPS, 0)
            acc = None
            for m in range(groups):
                t = vals[m] * e_row(l, m, o)
                acc = t if acc is None else acc + t
            ym_ref[l, o] = acc
            acc = None
            for j in range(pairs):
                t = vals[groups + j] * s_row(l, j, o)
                acc = t if acc is None else acc + t
            yst_ref[l, o] = acc
            return state

        lax.fori_loop(SWEEPS, hr - SWEEPS, second, start, unroll=UNROLL)
    lane = lax.broadcasted_iota(jnp.int32, (rows, cols), 1)
    for l in range(levels):
        main = jnp.sum(ym_ref[l, W:W + rows], axis=1)
        st = jnp.sum(yst_ref[l, W:W + rows], axis=1)
        st = st + pltpu.roll(st, HALF, 1)
        y_ref[l] = jnp.where((lane < W) | (lane >= cols - W), pltpu.roll(st, cols - 4 * W, 1), main)


def g_apply(e2, s2, gm, gs, wm, ws, dims):
    members, levels, rows, cols = dims
    hr = rows + 2 * W
    groups = members // 8
    pairs = groups // 2
    count = groups + pairs
    vm = pl.BlockSpec(memory_space=pltpu.VMEM)
    f32 = jnp.float32
    return pl.pallas_call(
        functools.partial(g_kernel, members=members, levels=levels, rows=rows, cols=cols),
        out_shape=(
            jax.ShapeDtypeStruct((levels * groups, hr, 8, cols), f32),
            jax.ShapeDtypeStruct((levels * pairs, hr, 8, cols), f32),
            jax.ShapeDtypeStruct((levels, rows, cols), f32),
        ),
        in_specs=[vm] * 6,
        out_specs=(vm,) * 3,
        scratch_shapes=[pltpu.VMEM((hr, cols), f32),
                        pltpu.VMEM((levels, hr, 8, cols), f32), pltpu.VMEM((levels, hr, 8, cols), f32),
                        pltpu.VMEM((count, hr, 8, cols), f32),
                        pltpu.VMEM((count, hr * 8, 2 * cols), jnp.bfloat16),
                        pltpu.VMEM((count, hr * 8, SWEEPS * cols), f32)],
        compiler_params=pltpu.CompilerParams(vmem_limit_bytes=60000000),
    )(e2, s2, gm, gs, wm, ws)


def sum_kernel(x_ref, o_ref, mid_ref, ra_ref, rb_ref, sa, qa, sb, qb):
    nx, ny = lax.axis_size("gx"), lax.axis_size("gy")
    mx, my = lax.axis_index("gx"), lax.axis_index("gy")
    bar = pltpu.get_barrier_semaphore()
    for axis, n, me in (("gx", nx, mx), ("gy", ny, my)):
        for k in range(1, n):
            pl.semaphore_signal(bar, inc=1, device_id={axis: lax.rem(me + k, n)}, device_id_type=pl.DeviceIdType.MESH)
    pl.semaphore_wait(bar, nx + ny - 2)

    def stage(axis, n, me, src, land, ssem, rsem):
        copies = []
        for k in range(1, n):
            copies.append(pltpu.make_async_remote_copy(
                src_ref=src, dst_ref=land.at[k - 1], send_sem=ssem.at[k - 1], recv_sem=rsem.at[k - 1],
                device_id={axis: lax.rem(me + k, n)}, device_id_type=pl.DeviceIdType.MESH))
            copies[-1].start()
        for c in copies:
            c.wait_recv()
        total = src[...]
        for k in range(n - 1):
            total = total + land[k]
        return copies, total

    ca, total = stage("gx", nx, mx, x_ref, ra_ref, sa, qa)
    mid_ref[...] = total
    cb, total = stage("gy", ny, my, mid_ref, rb_ref, sb, qb)
    o_ref[...] = total
    for c in ca + cb:
        c.wait_send()


def sum_all(x):
    nx, ny = lax.axis_size("gx"), lax.axis_size("gy")
    vm = pl.BlockSpec(memory_space=pltpu.VMEM)
    dma = pltpu.SemaphoreType.DMA
    return pl.pallas_call(
        sum_kernel,
        out_shape=jax.ShapeDtypeStruct(x.shape, x.dtype),
        in_specs=[vm],
        out_specs=vm,
        scratch_shapes=[pltpu.VMEM(x.shape, x.dtype), pltpu.VMEM((nx - 1,) + x.shape, x.dtype),
                        pltpu.VMEM((ny - 1,) + x.shape, x.dtype),
                        dma((nx - 1,)), dma((nx - 1,)), dma((ny - 1,)), dma((ny - 1,))],
        compiler_params=pltpu.CompilerParams(collective_id=0, has_side_effects=True),
    )(x)


def on_device(ensemble, obs_cell, obs_level, innovation, obs_weight):
    members, levels, rows, cols = ensemble.shape
    f32 = jnp.float32
    vm = pl.BlockSpec(memory_space=pltpu.VMEM)
    flat = lambda a: a.reshape(1, -1)
    e2, s2, g0, dd, gm, gs = prep(ensemble, flat(obs_cell), flat(obs_level), flat(innovation), flat(obs_weight))
    wm, ws = pl.pallas_call(
        functools.partial(weight_kernel, cols=cols),
        out_shape=(jax.ShapeDtypeStruct((2 * cols, SWEEPS * cols), jnp.bfloat16),) * 2,
        out_specs=(vm, vm),
    )()
    p0, ps0, y0 = g_apply(e2, s2, gm, gs, wm, ws, ensemble.shape)
    gm1, gs1 = next_state(y0, dd)
    p1, ps1, y1 = g_apply(e2, s2, gm1, gs1, wm, ws, ensemble.shape)
    sums = jnp.stack([jnp.sum(v, axis=(0, 1)) for v in (g0 * y0, dd * y0 * y0, dd * y0 * y1, dd * y1 * y1)])
    m = sum_all(jnp.concatenate([sums, jnp.zeros_like(sums)]))
    control, increment = pl.pallas_call(
        out_kernel,
        out_shape=(jax.ShapeDtypeStruct((members * levels * rows, cols), f32), jax.ShapeDtypeStruct((levels, rows, cols), f32)),
        in_specs=[vm] * 7,
        out_specs=(vm, vm),
        compiler_params=pltpu.CompilerParams(vmem_limit_bytes=60000000),
    )(m, p0, ps0, p1, ps1, y0, y1)
    return (control.reshape(members, levels, rows, cols), increment)


def solution(mesh):
    return jax.shard_map(
        on_device,
        mesh=mesh,
        in_specs=(
            P(None, None, "gy", "gx"),
            P("gy", "gx", None),
            P("gy", "gx", None),
            P("gy", "gx", None),
            P("gy", "gx", None),
        ),
        out_specs=(P(None, None, "gy", "gx"), P(None, "gy", "gx")),
        check_vma=False,
    )
```

```python
import functools
import math
import jax
import jax.numpy as jnp
from jax import lax
from jax.experimental import pallas as pl
from jax.experimental.pallas import tpu as pltpu
from jax.sharding import PartitionSpec as P

SWEEPS = 4
KAPPA = 0.2
EPS = 1e-06
W = 2 * SWEEPS
HALF = 64
UNROLL = 4


def scatter(cell_ref, level_ref, inn_ref, wt_ref, g_ref, d_ref):
    levels, rows, cols = g_ref.shape
    cell = cell_ref[...]
    row = level_ref[...] * rows + cell // cols
    col = cell % cols
    n = cell.shape[1]
    hot = jnp.where(lax.broadcasted_iota(jnp.int32, (levels * rows, n), 0) == row, 1.0, 0.0).astype(jnp.bfloat16)
    at = lax.broadcasted_iota(jnp.int32, (cols, n), 0) == col
    wt = wt_ref[...]
    for ref, v in ((g_ref, wt * inn_ref[...]), (d_ref, wt)):
        hi = v.astype(jnp.bfloat16).astype(jnp.float32)
        lo = v - hi
        total = None
        for part in (hi, lo):
            sel = jnp.where(at, part, 0.0).astype(jnp.bfloat16)
            term = lax.dot_general(hot, sel, (((1,), (1,)), ((), ())), preferred_element_type=jnp.float32)
            total = term if total is None else total + term
        for l in range(levels):
            ref[l] = total[l * rows:(l + 1) * rows]


SIDES = [(-1, 0), (1, 0), (0, -1), (0, 1), (-1, -1), (-1, 1), (1, -1), (1, 1)]


def peer(dy, dx):
    ny, nx = lax.axis_size("gy"), lax.axis_size("gx")
    return {"gy": lax.rem(lax.axis_index("gy") + dy + ny, ny), "gx": lax.rem(lax.axis_index("gx") + dx + nx, nx)}


def meet():
    bar = pltpu.get_barrier_semaphore()
    for dy, dx in SIDES:
        pl.semaphore_signal(bar, inc=1, device_id=peer(dy, dx), device_id_type=pl.DeviceIdType.MESH)
    total = len(SIDES)
    for axis in ("gx", "gy"):
        n, me = lax.axis_size(axis), lax.axis_index(axis)
        total += n - 1
        for k in range(1, n):
            pl.semaphore_signal(bar, inc=1, device_id={axis: lax.rem(me + k, n)}, device_id_type=pl.DeviceIdType.MESH)
    pl.semaphore_wait(bar, total)


def send_all(pairs, ssem, rsem):
    copies = []
    for n, ((dy, dx), (src, dst)) in enumerate(zip(SIDES, pairs)):
        copies.append(pltpu.make_async_remote_copy(
            src_ref=src, dst_ref=dst, send_sem=ssem.at[n], recv_sem=rsem.at[n],
            device_id=peer(dy, dx), device_id_type=pl.DeviceIdType.MESH))
        copies[-1].start()
    return copies


def pack_state(g_ref, pe_ref, pw_ref):
    levels, rows, cols = g_ref.shape
    block = lax.broadcasted_iota(jnp.int32, (8, cols), 1) // W
    e = w = jnp.zeros((8, cols), jnp.float32)
    per = rows // 8
    for l in range(levels):
        for t in range(per):
            p = l * per + t
            x = pltpu.roll(g_ref[l, t * 8:t * 8 + 8], (p * W + W) % cols, 1)
            e = jnp.where(block == p, x, e)
            w = jnp.where(block == (p + 1) % (cols // W), x, w)
    pe_ref[...] = e
    pw_ref[...] = w


def unpack_state(g_ref, land_n, land_p, gm_ref, gs_ref):
    levels, rows, cols = g_ref.shape
    hr = rows + 2 * W
    per = rows // 8
    lane = lax.broadcasted_iota(jnp.int32, (8, cols), 1)
    block = lane // W
    gy, gx = lax.axis_index("gy"), lax.axis_index("gx")
    c = strip_col(lane, cols) + gx * cols
    cok = (lane % HALF < 6 * W) & (c >= 0) & (c < cols * lax.axis_size("gx"))
    for l in range(levels):
        for t in range(-1, per + 1):
            if t < 0:
                x, pe, pw, p = land_n[1, l], land_p[5], land_p[4], l * per + per - 1
            elif t == per:
                x, pe, pw, p = land_n[0, l], land_p[3], land_p[2], l * per
            else:
                x, pe, pw, p = g_ref[l, t * 8:t * 8 + 8], land_p[1], land_p[0], l * per + t
            r = lax.broadcasted_iota(jnp.int32, (8, cols), 0) + gy * rows + t * 8
            rok = (r >= 0) & (r < rows * lax.axis_size("gy"))
            x = jnp.where(rok, x, 0.0)
            z = jnp.where(block == p, pe, pw)
            z1 = pltpu.roll(z, (cols - p * W) % cols, 1)
            z2 = pltpu.roll(z, (cols - p * W + HALF) % cols, 1)
            own = jnp.where(lane < HALF, pltpu.roll(x, 4 * W, 1), pltpu.roll(x, HALF + 4 * W, 1))
            halo = jnp.where(lane < HALF, z1, z2)
            gs = jnp.where(lane % HALF < 2 * W, halo, own)
            at = slice((t + 1) * 8, (t + 2) * 8)
            gm_ref[l, at] = x
            gs_ref[l, at] = jnp.where(rok & cok, gs, 0.0)


def state_pairs(g_ref, pe_ref, pw_ref, land_n, land_p):
    rows = g_ref.shape[1]
    return [(g_ref.at[:, 0:W], land_n.at[0]), (g_ref.at[:, rows - W:rows], land_n.at[1])] + [
        (pw_ref if dx < 0 else pe_ref, land_p.at[n]) for n, (dy, dx) in enumerate(SIDES[2:])]


def state_scratch(levels, cols):
    f32 = jnp.float32
    dma = pltpu.SemaphoreType.DMA
    return [pltpu.VMEM((8, cols), f32), pltpu.VMEM((8, cols), f32), pltpu.VMEM((2, levels, W, cols), f32),
            pltpu.VMEM((6, 8, cols), f32), dma((8,)), dma((8,))]


def prep_kernel(ens_ref, cell_ref, level_ref, inn_ref, wt_ref, e_ref, s_ref, g_ref, d_ref, gm_ref, gs_ref,
                wm_ref, ws_ref, ec_ref, pe_ref, pw_ref, en_ref, pee_ref, pew_ref, pc_ref, es, er,
                gpe, gpw, gn, gp, ss, sr):
    members, levels, rows, cols = ens_ref.shape
    hr = rows + 2 * W
    per = rows // 8
    pairs = members // 16
    lane = lax.broadcasted_iota(jnp.int32, (8, cols), 1)
    block = lane // W
    nb = cols // W

    def convert(k, x):
        for l in range(levels):
            ec_ref[k * levels + l] = ens_ref[k, l].astype(jnp.float32)
        return x

    lax.fori_loop(0, members, convert, 0)

    def pack(t, x):
        at = pl.ds(pl.multiple_of(t * 8, 8), 8)
        for l in range(levels):
            for j in range(pairs):
                e = w = jnp.zeros((8, cols), jnp.float32)
                for b in range(2):
                    for i in range(8):
                        p = b * 8 + i
                        x8 = pltpu.roll(ec_ref[(16 * j + p) * levels + l, at, :], (p * W + W) % cols, 1)
                        e = jnp.where(block == p, x8, e)
                        w = jnp.where(block == (p + 1) % nb, x8, w)
                pe_ref[l * pairs + j, at, :] = e
                pw_ref[l * pairs + j, at, :] = w
        return x

    lax.fori_loop(0, per, pack, 0)
    meet()
    top, bottom = slice(0, W), slice(rows - W, rows)
    jobs = [(ec_ref.at[:, top], en_ref.at[0]), (ec_ref.at[:, bottom], en_ref.at[1]), (pw_ref, pew_ref), (pe_ref, pee_ref)]
    for n, (dy, dx) in enumerate(SIDES[4:]):
        src = pw_ref if dx < 0 else pe_ref
        jobs.append((src.at[:, top if dy < 0 else bottom], pc_ref.at[n]))
    ecopies = send_all(jobs, es, er)
    scatter(cell_ref, level_ref, inn_ref, wt_ref, g_ref, d_ref)
    pack_state(g_ref, gpe, gpw)
    gcopies = send_all(state_pairs(g_ref, gpe, gpw, gn, gp), ss, sr)

    def center(f, x):
        e_ref[pl.ds(pl.multiple_of(f * hr + W, 8), rows), :] = ec_ref[f]
        return x

    lax.fori_loop(0, members * levels, center, 0)
    weight_kernel(wm_ref, ws_ref, cols=cols)
    for c in ecopies:
        c.wait_recv()

    def edges(f, x):
        e_ref[pl.ds(pl.multiple_of(f * hr, 8), W), :] = en_ref[1, f]
        e_ref[pl.ds(pl.multiple_of(f * hr + W + rows, 8), W), :] = en_ref[0, f]
        return x

    lax.fori_loop(0, members * levels, edges, 0)

    def strip_tile(lj, i, l, j, row, pe, pw):
        a = e_ref[pl.ds(pl.multiple_of(((16 * j + i) * levels + l) * hr + row, 8), 8), :]
        b = e_ref[pl.ds(pl.multiple_of(((16 * j + 8 + i) * levels + l) * hr + row, 8), 8), :]
        own = jnp.where(lane < HALF, pltpu.roll(a, 4 * W, 1), pltpu.roll(b, HALF + 4 * W, 1))
        z = pltpu.roll(jnp.where(block % 8 == i, pe, pw), (cols - i * W) % cols, 1)
        s_ref[pl.ds(pl.multiple_of((lj * 8 + i) * hr + row, 8), 8), :] = jnp.where(lane % HALF < 2 * W, z, own)

    for l in range(levels):
        for j in range(pairs):
            lj = l * pairs + j

            def mid(t, x):
                at = pl.ds(pl.multiple_of(t * 8, 8), 8)
                pe, pw = pee_ref[lj, at, :], pew_ref[lj, at, :]
                for i in range(8):
                    strip_tile(lj, i, l, j, W + t * 8, pe, pw)
                return x

            lax.fori_loop(0, per, mid, 0)
            for i in range(8):
                strip_tile(lj, i, l, j, 0, pc_ref[3, lj], pc_ref[2, lj])
                strip_tile(lj, i, l, j, W + rows, pc_ref[1, lj], pc_ref[0, lj])
    for c in gcopies:
        c.wait_recv()
    unpack_state(g_ref, gn, gp, gm_ref, gs_ref)
    for c in ecopies + gcopies:
        c.wait_send()


def next_kernel(y_ref, d_ref, gm_ref, gs_ref, g_ref, gpe, gpw, gn, gp, ss, sr):
    g_ref[...] = d_ref[...] * y_ref[...]
    pack_state(g_ref, gpe, gpw)
    copies = send_all(state_pairs(g_ref, gpe, gpw, gn, gp), ss, sr)
    for c in copies:
        c.wait_recv()
    unpack_state(g_ref, gn, gp, gm_ref, gs_ref)
    for c in copies:
        c.wait_send()


def out_kernel(m_ref, p0_ref, s0_ref, p1_ref, s1_ref, y0_ref, y1_ref, c_ref, inc_ref):
    levels, rows, cols = y0_ref.shape
    groups = p0_ref.shape[0] // levels
    pairs = groups // 2
    m = jnp.sum(m_ref[...], axis=1, keepdims=True)
    m = [m[k:k + 1] for k in range(4)]
    bn2 = m[0] + EPS
    c = (EPS - m[1]) / bn2
    alpha1 = (m[0] + m[1]) / bn2
    r2 = jnp.maximum((c * c * m[0] + 2.0 * c * m[1] + m[2]) / bn2, 0.0)
    rho = (c * c * m[1] + 2.0 * c * m[2] + m[3]) / bn2
    b2 = r2 + EPS
    alpha2 = (r2 + rho) / b2
    det = alpha1 * alpha2 - b2
    ca = jnp.broadcast_to((alpha2 - c) / det, (8, cols))
    cb = jnp.broadcast_to(-1.0 / det, (8, cols))
    for l in range(levels):
        for t in range(rows // 8):
            at = slice(t * 8, t * 8 + 8)
            inc_ref[l, at] = ca * y0_ref[l, at] + cb * y1_ref[l, at]
    lane = lax.broadcasted_iota(jnp.int32, (8, cols), 1)
    edge = (lane < W) | (lane >= cols - W)
    for l in range(levels):
        for j in range(pairs):
            def row(r, x):
                s = ca * s0_ref[l * pairs + j, W + r] + cb * s1_ref[l * pairs + j, W + r]
                for b in range(2):
                    g = l * groups + 2 * j + b
                    main = ca * p0_ref[g, W + r] + cb * p1_ref[g, W + r]
                    v = jnp.where(edge, pltpu.roll(s, (2 * cols - 4 * W - b * HALF) % cols, 1), main)
                    c_ref[pl.ds(((2 * j + b) * 8 * levels + l) * rows + r, 8, stride=levels * rows), :] = v
                return x

            lax.fori_loop(0, rows, row, 0, unroll=8)


def strip_col(lane, cols):
    lane = lane % HALF
    return jnp.where(lane < W, lane - W, jnp.where(lane < 2 * W, lane - W + cols,
                     jnp.where(lane < 4 * W, lane - 4 * W + cols, lane - 4 * W)))


def weight_kernel(wm_ref, ws_ref, *, cols):
    i = lax.broadcasted_iota(jnp.int32, (cols, cols), 0)
    j = lax.broadcasted_iota(jnp.int32, (cols, cols), 1)
    near = jnp.abs(i - j) <= 1
    gx = lax.axis_index("gx")

    def real(lane):
        c = strip_col(lane, cols) + gx * cols
        return (lane % HALF < 6 * W) & (c >= 0) & (c < cols * lax.axis_size("gx"))

    si, sj = strip_col(i, cols), strip_col(j, cols)
    same = ((i < HALF) == (j < HALF)) & (jnp.abs(si - sj) <= 1)

    for ref, ok in ((wm_ref, near), (ws_ref, same & real(i) & real(j))):
        one = jnp.where(ok, 1.0, 0.0).astype(jnp.bfloat16)
        power = one
        for s in range(1, SWEEPS + 1):
            if s > 1:
                power = jnp.dot(power, one, preferred_element_type=jnp.float32).astype(jnp.bfloat16)
            scaled = (power.astype(jnp.float32) * float(math.comb(SWEEPS, s))).astype(jnp.bfloat16)
            ref[0:cols, (s - 1) * cols:s * cols] = scaled
            ref[cols:2 * cols, (s - 1) * cols:s * cols] = scaled


def g_kernel(e_ref, s_ref, g_ref, gs_ref, wm_ref, ws_ref, p_ref, ps_ref, y_ref, km_ref, ym_ref, yst_ref,
             u_ref, lhs_ref, f_ref, *, members, levels, rows, cols):
    hr = rows + 2 * W
    groups = members // 8
    pairs = groups // 2
    count = groups + pairs
    scale = KAPPA ** SWEEPS
    gy = lax.axis_index("gy")
    rr = lax.broadcasted_iota(jnp.int32, (hr, cols), 0) + gy * rows - W
    km_ref[...] = jnp.where((rr >= 0) & (rr < rows * lax.axis_size("gy")), 1.0, 0.0)

    def e_row(l, m, r):
        return e_ref[pl.ds(((m * 8) * levels + l) * hr + r, 8, stride=levels * hr), :]

    def s_row(l, j, r):
        return s_ref[pl.ds(((l * pairs + j) * 8) * hr + r, 8, stride=hr), :]

    def ek_row(l, c, r):
        return e_row(l, c, r) if c < groups else s_row(l, c - groups, r)

    def split(c, r, u):
        hi = u.astype(jnp.bfloat16)
        lo = (u - hi.astype(jnp.float32)).astype(jnp.bfloat16)
        return hi, lo

    def products(lo_row, n):
        for c in range(count):
            w = wm_ref if c < groups else ws_ref
            f_ref[c, pl.ds(lo_row * 8, n * 8), :] = jnp.dot(
                lhs_ref[c, pl.ds(lo_row * 8, n * 8), :], w[...], preferred_element_type=jnp.float32)

    def sweep_all(state, vals, r):
        new = []
        for s in range(SWEEPS):
            o = jnp.maximum(r - s - 1, 0)
            km = km_ref[pl.ds(o, 1), :]
            out = []
            at = pl.ds(pl.multiple_of(o * 8, 8), 8)
            for c, u in enumerate(vals):
                older, prev = state[s][c]
                out.append(km * (older + u) + f_ref[c, at, s * cols:(s + 1) * cols])
                new.append((prev, u))
            vals = out
        return [new[s * count:(s + 1) * count] for s in range(SWEEPS)], [v * scale for v in vals]

    zero = km_ref[0:8, :] * 0.0
    start = [[(zero, zero)] * count for _ in range(SWEEPS)]
    step = hr

    def store_lhs(c, r, us):
        his, los = zip(*[split(c, r, u) for u in us])
        at = pl.ds(pl.multiple_of(r * 8, 16), 16)
        lhs_ref[c, at, 0:cols] = jnp.concatenate(his, axis=0)
        lhs_ref[c, at, cols:2 * cols] = jnp.concatenate(los, axis=0)

    for l in range(levels):
        def fill(i, carry):
            r = i * 2
            for c in range(count):
                us = []
                for k in range(2):
                    g = (g_ref if c < groups else gs_ref)[l, pl.ds(r + k, 1), :]
                    u = ek_row(l, c, r + k) * g
                    u_ref[c, r + k] = u
                    us.append(u)
                store_lhs(c, r, us)
            return carry

        lax.fori_loop(0, hr // 2, fill, 0, unroll=2)
        products(0, step)

        def first(r, state):
            state, vals = sweep_all(state, [u_ref[c, r] for c in range(count)], r)
            o = jnp.maximum(r - SWEEPS, 0)
            for m in range(groups):
                p_ref[l * groups + m, o] = vals[m]
            for j in range(pairs):
                ps_ref[l * pairs + j, o] = vals[groups + j]
            return state

        lax.fori_loop(0, hr, first, start, unroll=UNROLL)

        def refill(i, carry):
            r = i * 2
            for c in range(count):
                p = p_ref.at[l * groups + c] if c < groups else ps_ref.at[l * pairs + c - groups]
                store_lhs(c, r, [p[r], p[r + 1]])
            return carry

        lax.fori_loop(SWEEPS // 2, (hr - SWEEPS) // 2, refill, 0, unroll=2)
        products(0, step)

        def second(r, state):
            vals = [p_ref[l * groups + m, r] for m in range(groups)] + [ps_ref[l * pairs + j, r] for j in range(pairs)]
            state, vals = sweep_all(state, vals, r)
            o = jnp.maximum(r - SWEEPS, 0)
            acc = None
            for m in range(groups):
                t = vals[m] * e_row(l, m, o)
                acc = t if acc is None else acc + t
            ym_ref[l, o] = acc
            acc = None
            for j in range(pairs):
                t = vals[groups + j] * s_row(l, j, o)
                acc = t if acc is None else acc + t
            yst_ref[l, o] = acc
            return state

        lax.fori_loop(SWEEPS, hr - SWEEPS, second, start, unroll=UNROLL)
    lane = lax.broadcasted_iota(jnp.int32, (rows, cols), 1)
    for l in range(levels):
        main = jnp.sum(ym_ref[l, W:W + rows], axis=1)
        st = jnp.sum(yst_ref[l, W:W + rows], axis=1)
        st = st + pltpu.roll(st, HALF, 1)
        y_ref[l] = jnp.where((lane < W) | (lane >= cols - W), pltpu.roll(st, cols - 4 * W, 1), main)


def sum_kernel(x_ref, o_ref, mid_ref, ra_ref, rb_ref, sa, qa, sb, qb):
    nx, ny = lax.axis_size("gx"), lax.axis_size("gy")
    mx, my = lax.axis_index("gx"), lax.axis_index("gy")
    def stage(axis, n, me, src, land, ssem, rsem):
        copies = []
        for k in range(1, n):
            copies.append(pltpu.make_async_remote_copy(
                src_ref=src, dst_ref=land.at[k - 1], send_sem=ssem.at[k - 1], recv_sem=rsem.at[k - 1],
                device_id={axis: lax.rem(me + k, n)}, device_id_type=pl.DeviceIdType.MESH))
            copies[-1].start()
        for c in copies:
            c.wait_recv()
        total = src[...]
        for k in range(n - 1):
            total = total + land[k]
        return copies, total

    ca, total = stage("gx", nx, mx, x_ref, ra_ref, sa, qa)
    mid_ref[...] = total
    cb, total = stage("gy", ny, my, mid_ref, rb_ref, sb, qb)
    o_ref[...] = total
    for c in ca + cb:
        c.wait_send()


def whole_kernel(ens_ref, cell_ref, level_ref, inn_ref, wt_ref, c_ref, inc_ref,
                 e_ref, s_ref, g_ref, d_ref, gm_ref, gs_ref, wm_ref, ws_ref, p0, s0, y0, p1, s1, y1, g1_ref,
                 x_ref, m_ref, *rest):
    members, levels, rows, cols = ens_ref.shape
    dims = dict(members=members, levels=levels, rows=rows, cols=cols)
    ens_bufs, first_bufs, second_bufs, work, sum_bufs = rest[:9], rest[9:15], rest[15:21], rest[21:27], rest[27:]
    prep_kernel(ens_ref, cell_ref, level_ref, inn_ref, wt_ref, e_ref, s_ref, g_ref, d_ref, gm_ref, gs_ref,
                wm_ref, ws_ref, *ens_bufs, *first_bufs)
    g_kernel(e_ref, s_ref, gm_ref, gs_ref, wm_ref, ws_ref, p0, s0, y0, *work, **dims)
    next_kernel(y0, d_ref, gm_ref, gs_ref, g1_ref, *second_bufs)
    g_kernel(e_ref, s_ref, gm_ref, gs_ref, wm_ref, ws_ref, p1, s1, y1, *work, **dims)
    x_ref[...] = jnp.zeros_like(x_ref)
    for k, (a, b) in enumerate(((g_ref, y0), (g1_ref, y0), (g1_ref, y1), (None, y1))):
        v = d_ref[...] * y1[...] * y1[...] if a is None else a[...] * b[...]
        x_ref[k:k + 1, :] = jnp.sum(v.reshape(levels * rows, cols), axis=0, keepdims=True)
    sum_kernel(x_ref, m_ref, *sum_bufs)
    out_kernel(m_ref, p0, s0, p1, s1, y0, y1, c_ref, inc_ref)


def on_device(ensemble, obs_cell, obs_level, innovation, obs_weight):
    members, levels, rows, cols = ensemble.shape
    hr = rows + 2 * W
    f = members * levels
    groups = members // 8
    pairs = groups // 2
    count = groups + pairs
    q = levels * pairs
    nx, ny = lax.axis_size("gx"), lax.axis_size("gy")
    f32 = jnp.float32
    vm = pl.BlockSpec(memory_space=pltpu.VMEM)
    dma = pltpu.SemaphoreType.DMA
    v = lambda *s: pltpu.VMEM(s, f32)
    flat = lambda a: a.reshape(1, -1)
    image = [v(levels * groups, hr, 8, cols), v(levels * pairs, hr, 8, cols), v(levels, rows, cols)]
    weights = [pltpu.VMEM((2 * cols, SWEEPS * cols), jnp.bfloat16)] * 2
    control, increment = pl.pallas_call(
        whole_kernel,
        out_shape=(jax.ShapeDtypeStruct((f * rows, cols), f32), jax.ShapeDtypeStruct((levels, rows, cols), f32)),
        in_specs=[vm] * 5,
        out_specs=(vm, vm),
        scratch_shapes=[v(f * hr, cols), v(q * 8 * hr, cols), v(levels, rows, cols), v(levels, rows, cols),
                        v(levels, hr, cols), v(levels, hr, cols)] + weights + image + image
        + [v(levels, rows, cols), v(8, cols), v(8, cols)]
        + [v(f, rows, cols), v(q, rows, cols), v(q, rows, cols), v(2, f, W, cols), v(q, rows, cols), v(q, rows, cols),
           v(4, q, W, cols), dma((8,)), dma((8,))]
        + state_scratch(levels, cols) + state_scratch(levels, cols)
        + [v(hr, cols), v(levels, hr, 8, cols), v(levels, hr, 8, cols), v(count, hr, 8, cols),
           pltpu.VMEM((count, hr * 8, 2 * cols), jnp.bfloat16), v(count, hr * 8, SWEEPS * cols)]
        + [v(8, cols), v(nx - 1, 8, cols), v(ny - 1, 8, cols), dma((nx - 1,)), dma((nx - 1,)), dma((ny - 1,)), dma((ny - 1,))],
        compiler_params=pltpu.CompilerParams(collective_id=0, has_side_effects=True, vmem_limit_bytes=64000000),
    )(ensemble, flat(obs_cell), flat(obs_level), flat(innovation), flat(obs_weight))
    return (control.reshape(members, levels, rows, cols), increment)


def solution(mesh):
    return jax.shard_map(
        on_device,
        mesh=mesh,
        in_specs=(
            P(None, None, "gy", "gx"),
            P("gy", "gx", None),
            P("gy", "gx", None),
            P("gy", "gx", None),
            P("gy", "gx", None),
        ),
        out_specs=(P(None, None, "gy", "gx"), P(None, "gy", "gx")),
        check_vma=False,
    )
```
